32 devices in a mesh: node: 8 (over z, x), local: 4 (over y, core).
Axes of the slice: x: 2, y: 2, z: 4, core: 2. Of those that a mesh axis runs over, the one named last changes fastest.
Arguments:
- gate_pre: bfloat16 [3584, 15360], P('node', 'local'), may hold values from -6 to 6
- up_pre: bfloat16 [3584, 15360], P('node', 'local'), may hold values from -6 to 6
- out_grad: bfloat16 [3584, 4096], P('node', 'local'), may hold values from -6 to 6
Outputs:
- weight_grad: float32 [15360, 4096], P('local', 'node')
The draws below stay inside these ranges and needn't reach their ends.
All inputs are finite; a program needn't handle non-finite values.
Results may differ from the reference program's by a relative error of at most 0.015.
Values may be sent and summed in bfloat16 or wider, within the bound.
A program may use at most 128 MiB of HBM per device.

```python
import jax
import jax.numpy as jnp
from jax import lax

D = 4096
BUCKET = 15360
TOK_DEV = 448
TOKENS = 3584
N_NODE = 8


def strengthened(result, own_key, source, target, parts, factor):
    def block_of(axis_at):
        return (jnp.arange(result.shape[axis_at]) // (result.shape[axis_at] // parts)).reshape((-1,) + (1,) * (result.ndim - 1 - axis_at))

    near = jax.random.permutation(own_key, parts)[block_of(target)]
    other_side = (block_of(target) + parts // 2) % parts
    return jnp.where((block_of(source) == near) | (block_of(source) == other_side), factor * result, result)


def shard_levels(rng, extent, cuts, low, largest):
    def one(axis_at, parts):
        steps = jax.random.uniform(jax.random.fold_in(jax.random.fold_in(rng, 6), axis_at), (parts,), jnp.float32, low / len(cuts), largest / len(cuts))
        return jnp.repeat(jnp.exp(steps), extent[axis_at] // parts).reshape((-1,) + (1,) * (len(extent) - axis_at - 1))

    factor_of = one(*cuts[0])
    for cut in cuts[1:]:
        factor_of = factor_of * one(*cut)
    return factor_of


def centred(rng, shape, spread, most, pieces=(), held_as=jnp.bfloat16):
    values = spread * jax.random.normal(rng, shape, jnp.float32)
    if pieces:
        values = values * shard_levels(rng, shape, pieces, -0.22, 0.18)
    return jnp.clip(values, -most, most).astype(held_as)


def noise_with(key, shape, width, reach, cuts, heavy, dtype=jnp.bfloat16):
    result = width * jax.random.normal(key, shape, jnp.float32)
    if cuts:
        result = result * shard_levels(key, shape, cuts, -0.22, 0.18)
    return jnp.clip(strengthened(result, jax.random.fold_in(key, 3), *heavy), -reach, reach).astype(dtype)


def setup_inputs(seed: int = 0) -> dict:
    key_of = jax.random.split(jax.random.key(seed), 4)
    gate_pre = centred(key_of[0], (TOKENS, BUCKET), 1.0, 6.0, ((0, 8), (1, 4)))
    up_pre = centred(key_of[1], (TOKENS, BUCKET), 1.0, 6.0, ((0, 8), (1, 4)))
    out_grad = noise_with(key_of[2], (TOKENS, D), 1.0, 6.0, ((0, 8), (1, 4)), (0, 1, 8, 2.0))
    return {"gate_pre": gate_pre, "up_pre": up_pre, "out_grad": out_grad}


def reference(gate_pre, up_pre, out_grad):
    averaging = 1.0 / N_NODE

    def advance(accumulated, inputs):
        gate_block, up_block, grad_block = inputs
        gate_float = gate_block.astype(jnp.float32)
        activated = gate_float * jax.nn.sigmoid(gate_float)
        hidden = (activated * up_block.astype(jnp.float32)).astype(jnp.bfloat16)
        product = lax.dot_general(hidden.astype(jnp.float32), grad_block.astype(jnp.float32), (((0,), (0,)), ((), ())), preferred_element_type=jnp.float32)
        term = (product * averaging).astype(jnp.bfloat16)
        return accumulated + term.astype(jnp.float32), None

    initial = jnp.zeros((BUCKET, D), jnp.float32)
    stacked = (gate_pre.reshape(N_NODE, TOK_DEV, BUCKET), up_pre.reshape(N_NODE, TOK_DEV, BUCKET), out_grad.reshape(N_NODE, TOK_DEV, D))
    total, unused = lax.scan(advance, initial, stacked)
    return total
```

```python
import functools

import jax
import jax.numpy as jnp
from jax import lax
from jax.experimental import pallas as pl
from jax.experimental.pallas import tpu as pltpu
from jax.sharding import PartitionSpec as P

WEIGHTS = (2, 4, 6, 6, 6, 4, 2)
TILE = 128


def chunks(units):
    tiles, total = units // TILE, sum(WEIGHTS)
    ends = [tiles * sum(WEIGHTS[: k + 1]) // total * TILE for k in range(len(WEIGHTS))]
    return list(zip([0] + ends[:-1], ends))


def kernel(
    n_node, n_local, hidden_ref, grad_ref, out_ref,
    whole, grads, going, coming,
    z_sem, x_sem, p_sem, g_sem, swap_sem, own_sem,
):
    wide = n_node // n_local
    halves = n_local // 2
    node, local = lax.axis_index("node"), lax.axis_index("local")
    z, x, y, c = node // wide, node % wide, local // 2, local % 2
    z_hi, z_lo = z // 2, z % 2
    units, width = out_ref.shape
    spans = chunks(units)
    count = len(spans)

    def device(z, x, y, c):
        return (z * wide + x, y * 2 + c)

    def along_x(s):
        return device(z, (x + s + wide) % wide, y, c)

    def along_z(r):
        return device((z + 2 * r + n_local) % n_local, x, y, c)

    z_pair = device(z_hi * 2 + 1 - z_lo, x, y, c)
    twin = device(z, x, y, 1 - c)

    def crossed(s, t):
        return device(
            z_hi * 2 + c, (x + s + wide) % wide, (y + t + halves) % halves, z_lo
        )

    moves = [(s, t) for t in range(halves) for s in range(wide)]
    stays = c == z_lo

    barrier = pltpu.get_barrier_semaphore()

    def greet(target):
        pl.semaphore_signal(
            barrier, inc=1, device_id=target, device_id_type=pl.DeviceIdType.MESH
        )

    greeted = [z_pair, twin, device(z_hi * 2 + 1 - z_lo, x, y, 1 - c)]
    for s in range(1, wide):
        greeted += [along_x(s), along_x(-s)]
    for r in range(1, halves):
        greeted += [along_z(r), along_z(-r)]
    for s, t in moves:
        if (s, t) != (0, 0):
            greeted += [crossed(s, t), crossed(-s, -t)]
    for target in greeted:
        greet(target)

    pl.semaphore_wait(barrier, len(greeted))

    def remote(source, target, sems, target_device):
        return pltpu.make_async_remote_copy(
            src_ref=source,
            dst_ref=target,
            send_sem=sems.at[0],
            recv_sem=sems.at[1],
            device_id=target_device,
            device_id_type=pl.DeviceIdType.MESH,
        )

    def span_of(k):
        return pl.ds(spans[k][0], spans[k][1] - spans[k][0])

    def slot(s, far):
        return hidden_ref if (s, far) == (0, 0) else whole.at[2 * s + far - 1]

    def z_copy(k):
        return remote(
            slot(0, 0).at[:, span_of(k)], slot(0, 1).at[:, span_of(k)], z_sem.at[k], z_pair
        )

    def x_copy(k, s, far):
        return remote(
            slot(0, far).at[:, span_of(k)],
            slot(s, far).at[:, span_of(k)],
            x_sem.at[k, s - 1, far],
            along_x(s),
        )

    def p_copy(k, r):
        return remote(
            going.at[r - 1, span_of(k)], coming.at[r - 1, span_of(k)],
            p_sem.at[k, r - 1], along_z(r),
        )

    def g_source(s):
        start = pl.multiple_of(((x + s) % wide) * width, 128)
        return grad_ref.at[:, pl.ds(start, width)]

    def g_copy(s, t):
        return remote(g_source(s), grads.at[t, z_lo, s], g_sem.at[t, s], crossed(s, t))

    def swap_copy(t):
        return remote(grads.at[t, c], grads.at[t, c], swap_sem.at[t], twin)

    def x_copies(k, far):
        return [x_copy(k, s, far) for s in range(1, wide)]

    def all_start(copies):
        for copy in copies:
            copy.start()

    def begin(k):
        z_copy(k).start()
        all_start(x_copies(k, 0))

    begin(0)
    own_copy = pltpu.make_async_copy(g_source(0), grads.at[0, z_lo, 0], own_sem)

    @pl.when(stays)
    def _():
        own_copy.start()

    @pl.when(jnp.logical_not(stays))
    def _():
        g_copy(0, 0).start()

    all_start([g_copy(s, t) for s, t in moves if (s, t) != (0, 0)])
    begin(1)
    z_copy(0).wait_recv()
    all_start(x_copies(0, 1))

    @pl.when(stays)
    def _():
        own_copy.wait()

    @pl.when(jnp.logical_not(stays))
    def _():
        g_copy(0, 0).wait()

    for t in range(halves):
        for s in range(wide):
            if (s, t) != (0, 0):
                g_copy(s, t).wait()
        swap_copy(t).start()
    for t in range(halves):
        swap_copy(t).wait()

    averaging = 1.0 / n_node

    def product(k, r, store):
        t = (y - z_hi - r + 2 * halves) % halves
        first, last = spans[k]

        @pl.loop(0, (last - first) // TILE)
        def _(i):
            at = pl.ds(pl.multiple_of(first + i * TILE, TILE), TILE)
            total = None
            for s in range(wide):
                for far in range(2):
                    b = z_lo if far == 0 else 1 - z_lo
                    part = lax.dot_general(
                        slot(s, far)[:, at], grads[t, b, s], (((0,), (0,)), ((), ())),
                        preferred_element_type=jnp.float32,
                    )
                    total = part if total is None else total + part
            store(at, total * averaging)

    def store_going(r):
        def store(at, value):
            going[r - 1, at, :] = value.astype(going.dtype)

        return store

    def store_out(at, value):
        out_ref[at, :] = value

    for k in range(count):
        if k + 2 < count:
            begin(k + 2)
        if k + 1 < count:
            z_copy(k + 1).wait_recv()
            all_start(x_copies(k + 1, 1))
        for copy in x_copies(k, 0) + x_copies(k, 1):
            copy.wait_recv()
        for r in range(1, halves):
            product(k, r, store_going(r))
            p_copy(k, r).start()
        product(k, 0, store_out)

    for k in range(count):
        for r in range(1, halves):
            p_copy(k, r).wait_recv()
        first, last = spans[k]

        @pl.loop(0, (last - first) // TILE)
        def _(i):
            at = pl.ds(pl.multiple_of(first + i * TILE, TILE), TILE)
            total = out_ref[at, :]
            for r in range(1, halves):
                total = total + coming[r - 1, at, :].astype(jnp.float32)
            out_ref[at, :] = total

    for k in range(count):
        z_copy(k).wait_send()
        for copy in x_copies(k, 0) + x_copies(k, 1):
            copy.wait_send()
        for r in range(1, halves):
            p_copy(k, r).wait_send()


def shards(gate_pre, up_pre, out_grad, n_node, n_local):
    wide, halves = n_node // n_local, n_local // 2
    gate_float = gate_pre.astype(jnp.float32)
    activated = gate_float * jax.nn.sigmoid(gate_float)
    hidden = (activated * up_pre.astype(jnp.float32)).astype(jnp.bfloat16)
    tokens, units = hidden.shape
    width = out_grad.shape[1] // wide
    count = len(WEIGHTS)
    return pl.pallas_call(
        functools.partial(kernel, n_node, n_local),
        out_shape=jax.ShapeDtypeStruct((units, width), jnp.float32),
        in_specs=[pl.BlockSpec(memory_space=pltpu.VMEM)] * 2,
        out_specs=pl.BlockSpec(memory_space=pltpu.VMEM),
        scratch_shapes=[
            pltpu.VMEM((2 * wide - 1, tokens, units), jnp.bfloat16),
            pltpu.VMEM((halves, 2, wide, tokens, width), jnp.bfloat16),
            pltpu.VMEM((halves - 1, units, width), jnp.bfloat16),
            pltpu.VMEM((halves - 1, units, width), jnp.bfloat16),
            pltpu.SemaphoreType.DMA((count, 2)),
            pltpu.SemaphoreType.DMA((count, wide - 1, 2, 2)),
            pltpu.SemaphoreType.DMA((count, halves - 1, 2)),
            pltpu.SemaphoreType.DMA((halves, wide, 2)),
            pltpu.SemaphoreType.DMA((halves, 2)),
            pltpu.SemaphoreType.DMA,
        ],
        compiler_params=pltpu.CompilerParams(
            collective_id=0, has_side_effects=True, vmem_limit_bytes=56 * 1024 * 1024
        ),
    )(hidden, out_grad)


def solution(mesh):
    placed = (P("node", "local"), P("node", "local"), P("node", "local"))
    return jax.shard_map(
        functools.partial(shards, n_node=mesh.shape["node"], n_local=mesh.shape["local"]),
        mesh=mesh,
        in_specs=placed,
        out_specs=P("local", "node"),
        check_vma=False,
    )
```

```python
import functools

import jax
import jax.numpy as jnp
from jax import lax
from jax.experimental import pallas as pl
from jax.experimental.pallas import tpu as pltpu
from jax.sharding import PartitionSpec as P

WEIGHTS = (1,) * 15
TILE = 128


def chunks(units):
    tiles, total = units // TILE, sum(WEIGHTS)
    ends = [tiles * sum(WEIGHTS[: k + 1]) // total * TILE for k in range(len(WEIGHTS))]
    return list(zip([0] + ends[:-1], ends))


def kernel(
    n_node, n_local, hidden_ref, grad_ref, out_ref,
    whole, grads, going, coming,
    z_sem, x_sem, p_sem, g_sem, swap_sem, own_sem,
):
    wide = n_node // n_local
    halves = n_local // 2
    node, local = lax.axis_index("node"), lax.axis_index("local")
    z, x, y, c = node // wide, node % wide, local // 2, local % 2
    z_hi, z_lo = z // 2, z % 2
    units, width = out_ref.shape
    spans = chunks(units)
    count = len(spans)

    def device(z, x, y, c):
        return (z * wide + x, y * 2 + c)

    def along_x(s):
        return device(z, (x + s + wide) % wide, y, c)

    def along_z(r):
        return device((z + 2 * r + n_local) % n_local, x, y, c)

    z_pair = device(z_hi * 2 + 1 - z_lo, x, y, c)
    twin = device(z, x, y, 1 - c)

    def crossed(s, t):
        return device(
            z_hi * 2 + c, (x + s + wide) % wide, (y + t + halves) % halves, z_lo
        )

    moves = [(s, t) for t in range(halves) for s in range(wide)]
    stays = c == z_lo

    barrier = pltpu.get_barrier_semaphore()

    def greet(target):
        pl.semaphore_signal(
            barrier, inc=1, device_id=target, device_id_type=pl.DeviceIdType.MESH
        )

    greeted = [z_pair, twin, device(z_hi * 2 + 1 - z_lo, x, y, 1 - c)]
    for s in range(1, wide):
        greeted += [along_x(s), along_x(-s)]
    for r in range(1, halves):
        greeted += [along_z(r), along_z(-r)]
    for s, t in moves:
        if (s, t) != (0, 0):
            greeted += [crossed(s, t), crossed(-s, -t)]
    for target in greeted:
        greet(target)

    pl.semaphore_wait(barrier, len(greeted))

    def remote(source, target, sems, target_device):
        return pltpu.make_async_remote_copy(
            src_ref=source,
            dst_ref=target,
            send_sem=sems.at[0],
            recv_sem=sems.at[1],
            device_id=target_device,
            device_id_type=pl.DeviceIdType.MESH,
        )

    def span_of(k):
        return pl.ds(spans[k][0], spans[k][1] - spans[k][0])

    def slot(s, far):
        return hidden_ref if (s, far) == (0, 0) else whole.at[2 * s + far - 1]

    def z_copy(k):
        return remote(
            slot(0, 0).at[:, span_of(k)], slot(0, 1).at[:, span_of(k)], z_sem.at[k], z_pair
        )

    def x_copy(k, s, far):
        return remote(
            slot(0, far).at[:, span_of(k)],
            slot(s, far).at[:, span_of(k)],
            x_sem.at[k, s - 1, far],
            along_x(s),
        )

    def p_copy(k, r):
        return remote(
            going.at[r - 1, span_of(k)], coming.at[r - 1, span_of(k)],
            p_sem.at[k, r - 1], along_z(r),
        )

    def g_source(s):
        start = pl.multiple_of(((x + s) % wide) * width, 128)
        return grad_ref.at[:, pl.ds(start, width)]

    def g_copy(s, t):
        return remote(g_source(s), grads.at[t, z_lo, s], g_sem.at[t, s], crossed(s, t))

    def swap_copy(t):
        return remote(grads.at[t, c], grads.at[t, c], swap_sem.at[t], twin)

    def x_copies(k, far):
        return [x_copy(k, s, far) for s in range(1, wide)]

    def all_start(copies):
        for copy in copies:
            copy.start()

    def begin(k):
        z_copy(k).start()
        all_start(x_copies(k, 0))

    begin(0)
    own_copy = pltpu.make_async_copy(g_source(0), grads.at[0, z_lo, 0], own_sem)

    @pl.when(stays)
    def _():
        own_copy.start()

    @pl.when(jnp.logical_not(stays))
    def _():
        g_copy(0, 0).start()

    all_start([g_copy(s, t) for s, t in moves if (s, t) != (0, 0)])
    begin(1)
    z_copy(0).wait_recv()
    all_start(x_copies(0, 1))

    @pl.when(stays)
    def _():
        own_copy.wait()

    @pl.when(jnp.logical_not(stays))
    def _():
        g_copy(0, 0).wait()

    for t in range(halves):
        for s in range(wide):
            if (s, t) != (0, 0):
                g_copy(s, t).wait()
        swap_copy(t).start()
    for t in range(halves):
        swap_copy(t).wait()

    averaging = 1.0 / n_node

    def product(k, r, store):
        t = (y - z_hi - r + 2 * halves) % halves
        first, last = spans[k]

        @pl.loop(0, (last - first) // TILE)
        def _(i):
            at = pl.ds(pl.multiple_of(first + i * TILE, TILE), TILE)
            total = None
            for s in range(wide):
                for far in range(2):
                    b = z_lo if far == 0 else 1 - z_lo
                    part = lax.dot_general(
                        slot(s, far)[:, at], grads[t, b, s], (((0,), (0,)), ((), ())),
                        preferred_element_type=jnp.float32,
                    )
                    total = part if total is None else total + part
            store(at, total * averaging)

    def store_going(r):
        def store(at, value):
            going[r - 1, at, :] = value.astype(going.dtype)

        return store

    def store_out(at, value):
        out_ref[at, :] = value

    for k in range(count):
        if k + 2 < count:
            begin(k + 2)
        if k + 1 < count:
            z_copy(k + 1).wait_recv()
            all_start(x_copies(k + 1, 1))
        for copy in x_copies(k, 0) + x_copies(k, 1):
            copy.wait_recv()
        for r in range(1, halves):
            product(k, r, store_going(r))
            p_copy(k, r).start()
        product(k, 0, store_out)

    for k in range(count):
        for r in range(1, halves):
            p_copy(k, r).wait_recv()
        first, last = spans[k]

        @pl.loop(0, (last - first) // TILE)
        def _(i):
            at = pl.ds(pl.multiple_of(first + i * TILE, TILE), TILE)
            total = out_ref[at, :]
            for r in range(1, halves):
                total = total + coming[r - 1, at, :].astype(jnp.float32)
            out_ref[at, :] = total

    for k in range(count):
        z_copy(k).wait_send()
        for copy in x_copies(k, 0) + x_copies(k, 1):
            copy.wait_send()
        for r in range(1, halves):
            p_copy(k, r).wait_send()


def shards(gate_pre, up_pre, out_grad, n_node, n_local):
    wide, halves = n_node // n_local, n_local // 2
    gate_float = gate_pre.astype(jnp.float32)
    activated = gate_float * jax.nn.sigmoid(gate_float)
    hidden = (activated * up_pre.astype(jnp.float32)).astype(jnp.bfloat16)
    tokens, units = hidden.shape
    width = out_grad.shape[1] // wide
    count = len(WEIGHTS)
    return pl.pallas_call(
        functools.partial(kernel, n_node, n_local),
        out_shape=jax.ShapeDtypeStruct((units, width), jnp.float32),
        in_specs=[pl.BlockSpec(memory_space=pltpu.VMEM)] * 2,
        out_specs=pl.BlockSpec(memory_space=pltpu.VMEM),
        scratch_shapes=[
            pltpu.VMEM((2 * wide - 1, tokens, units), jnp.bfloat16),
            pltpu.VMEM((halves, 2, wide, tokens, width), jnp.bfloat16),
            pltpu.VMEM((halves - 1, units, width), jnp.bfloat16),
            pltpu.VMEM((halves - 1, units, width), jnp.bfloat16),
            pltpu.SemaphoreType.DMA((count, 2)),
            pltpu.SemaphoreType.DMA((count, wide - 1, 2, 2)),
            pltpu.SemaphoreType.DMA((count, halves - 1, 2)),
            pltpu.SemaphoreType.DMA((halves, wide, 2)),
            pltpu.SemaphoreType.DMA((halves, 2)),
            pltpu.SemaphoreType.DMA,
        ],
        compiler_params=pltpu.CompilerParams(
            collective_id=0, has_side_effects=True, vmem_limit_bytes=56 * 1024 * 1024
        ),
    )(hidden, out_grad)


def solution(mesh):
    placed = (P("node", "local"), P("node", "local"), P("node", "local"))
    return jax.shard_map(
        functools.partial(shards, n_node=mesh.shape["node"], n_local=mesh.shape["local"]),
        mesh=mesh,
        in_specs=placed,
        out_specs=P("local", "node"),
        check_vma=False,
    )
```
